128 devices in a mesh: gx: 4 (over z), gy: 32 (over y, x, core).
Axes of the slice: x: 4, y: 4, z: 4, core: 2. Of those that a mesh axis runs over, the one named last changes fastest.
Arguments:
- radiance: bfloat16 [8192, 16, 128], P(('gx', 'gy')), may hold values from 0.049804688 to 2
- emission: float32 [8192, 16, 128], P(('gx', 'gy')), may hold values from 0.01 to 1
- reflectance: float32 [8192, 16, 128], P(('gx', 'gy')), may hold values from 0.1 to 0.9
- patch_area: float32 [8192, 128], P(('gx', 'gy')), may hold values from 0.25 to 4
- form_factor: bfloat16 [65536, 128, 128], P(('gx', 'gy')), may hold values from 0.00049972534 to 0.014953613
- source_index: int32 [128, 512], P(('gx', 'gy')), may hold values from 0 to 63
- target_index: int32 [128, 512], P(('gx', 'gy')), may hold values from 0 to 63
- block_index: int32 [128, 512], P(('gx', 'gy')), may hold values from 0 to 511, each once within a row
- valid_count: int32 [128, 128], P(('gx', 'gy')), may hold values from 0 to 4, as said below
Outputs:
- new_radiance: float32 [8192, 16, 128], P(('gx', 'gy'))
The draws below stay inside these ranges and needn't reach their ends.
Inputs may be any that keep to these rules, and one draw needn't show every extreme that they name: `valid_count`: entry [d, p] is the number of live slots among the 4 slots of device d toward peer p, the live ones first; every row has an entry equal to 4. `block_index`: each row is a permutation of 0 to 511.
All inputs are finite; a program needn't handle non-finite values.
Results may differ from the reference program's by a relative error of at most 0.0012.
Values may be sent and summed in bfloat16 or wider, within the bound.
A program may use at most 128 MiB of HBM per device.

```python
import math
import jax
import jax.numpy as jnp
from jax import lax

PATCH = 128
BANDS = 16
CL_DEV = 64
SLOTS = 4
CLUSTERS = 8192
LINKS = 512
DEVICES = 128


def draw_valid_count(key, part):
    base_key = jax.random.fold_in(key, 7)
    heavy_key, count_key, full_key = jax.random.split(base_key, 3)
    heavy_flag = jax.random.randint(heavy_key, (DEVICES, 1), 0, 4) == 0
    lowest = jnp.where(heavy_flag, SLOTS // 2, 0)
    highest = jnp.where(heavy_flag, SLOTS, SLOTS // 2)
    raw_bits = jax.random.randint(count_key, (DEVICES, DEVICES), 0, 1 << 20)
    counts = lowest + raw_bits % (highest - lowest + 1)
    full_peer = jax.random.randint(full_key, (DEVICES,), 0, DEVICES)
    columns = jnp.arange(DEVICES, dtype=jnp.int32)
    counts = jnp.where(columns[None, :] == full_peer[:, None], SLOTS, counts)
    return counts.astype(jnp.int32)


def place_ends(array, rng, smallest, top_value):
    spot = [jax.random.randint(jax.random.fold_in(rng, axis), (), 0, length) for axis, length in enumerate(array.shape)]
    main_axis = array.shape.index(max(array.shape))
    next_to = spot[:main_axis] + [(spot[main_axis] + 1) % array.shape[main_axis]] + spot[main_axis + 1:]
    return array.at[tuple(spot)].set(smallest).at[tuple(next_to)].set(top_value)


def levels(own_key, shape, cuts, low, top_value):
    loudness = 1.0
    for axis_at, shards_of in cuts:
        steps = jax.random.uniform(jax.random.fold_in(jax.random.fold_in(own_key, 6), axis_at), (shards_of,), jnp.float32, low / len(cuts), top_value / len(cuts))
        loudness = loudness * jnp.repeat(jnp.exp(steps), shape[axis_at] // shards_of).reshape((-1,) + (1,) * (len(shape) - 1 - axis_at))
    return loudness


def setup_inputs(seed: int = 0) -> dict:
    seeds = jax.random.split(jax.random.key(seed), 10)
    return {
        "radiance": jnp.clip(jnp.exp(math.log(2.0) - 3.6927934 * jax.random.uniform(seeds[0], (CLUSTERS, BANDS, PATCH), jnp.float32) ** levels(seeds[0], (CLUSTERS, BANDS, PATCH), ((0, 128),), -0.2, 0.2)), 0.049804688, 2.0).astype(jnp.bfloat16),
        "emission": jnp.clip(jnp.exp(math.log(1.0) - 4.6051702 * jax.random.uniform(seeds[1], (CLUSTERS, BANDS, PATCH), jnp.float32) ** levels(seeds[1], (CLUSTERS, BANDS, PATCH), ((0, 128),), -0.2, 0.2)), 0.01, 1.0),
        "reflectance": jnp.clip(jnp.exp(math.log(0.9) - 2.1972245 * jax.random.uniform(seeds[2], (CLUSTERS, BANDS, PATCH), jnp.float32) ** levels(seeds[2], (CLUSTERS, BANDS, PATCH), ((0, 128),), -0.2, 0.2)), 0.1, 0.9),
        "patch_area": jnp.clip(jnp.exp(math.log(4.0) - 2.7725887 * jax.random.uniform(seeds[3], (CLUSTERS, PATCH), jnp.float32) ** levels(seeds[3], (CLUSTERS, PATCH), ((0, 128),), -0.2, 0.2)), 0.25, 4.0),
        "form_factor": jnp.clip(jnp.exp(math.log(0.014953613) - 3.3986496 * jax.random.uniform(seeds[4], (DEVICES * LINKS, PATCH, PATCH), jnp.float32) ** levels(seeds[4], (DEVICES * LINKS, PATCH, PATCH), ((0, 128),), -0.2, 0.2)), 0.00049972534, 0.014953613).astype(jnp.bfloat16),
        "source_index": place_ends(jax.random.randint(seeds[5], (DEVICES, LINKS), 0, CL_DEV), jax.random.fold_in(seeds[5], 1), 0, CL_DEV - 1).astype(jnp.int32),
        "target_index": place_ends(jax.random.randint(seeds[6], (DEVICES, LINKS), 0, CL_DEV), jax.random.fold_in(seeds[6], 1), 0, CL_DEV - 1).astype(jnp.int32),
        "block_index": jax.vmap(lambda own: jax.random.permutation(own, LINKS))(jax.random.split(seeds[7], DEVICES)).reshape((DEVICES, LINKS)).astype(jnp.int32),
        "valid_count": draw_valid_count(jax.random.fold_in(seeds[9], 71), 0),
    }


def reference(radiance, emission, reflectance, patch_area, form_factor, source_index, target_index, block_index, valid_count):
    rad_full = radiance.astype(jnp.float32)
    weighted = (patch_area[:, None, :] * rad_full).astype(jnp.bfloat16)
    weighted_full = weighted.astype(jnp.float32)
    blocks = form_factor.reshape(DEVICES, LINKS, PATCH, PATCH)
    device_ids = jnp.arange(DEVICES, dtype=jnp.int32)

    def step_device(carry, inputs):
        gathered, returned = carry
        device, block_row, source_row, target_row, stored_blocks, live_count = inputs
        position = jnp.arange(LINKS, dtype=jnp.int32)
        peer_ids = (position // SLOTS).astype(jnp.int32)
        live_mask = ((position % SLOTS) < live_count[peer_ids]).astype(jnp.float32)
        source_cluster = (peer_ids * CL_DEV + source_row).astype(jnp.int32)
        target_cluster = (device * CL_DEV + target_row).astype(jnp.int32)
        chosen = stored_blocks[block_row].astype(jnp.float32)
        forward = jnp.einsum("lij,lbj->lbi", chosen, rad_full[source_cluster]) * live_mask[:, None, None]
        backward = jnp.einsum("lij,lbi->lbj", chosen, weighted_full[target_cluster]).astype(jnp.bfloat16)
        backward = lax.optimization_barrier(backward)
        backward = backward.astype(jnp.float32) * live_mask[:, None, None]
        gathered = gathered.at[target_cluster].add(forward)
        returned = returned.at[source_cluster].add(backward)
        return (gathered, returned), None

    zeros_sum = jnp.zeros((CLUSTERS, BANDS, PATCH), jnp.float32)
    (gathered, returned), _ = lax.scan(step_device, (zeros_sum, zeros_sum),
                                       (device_ids, block_index, source_index, target_index, blocks, valid_count))
    irradiance = gathered + returned / patch_area[:, None, :]
    return emission + reflectance * irradiance
```

```python
import functools

import jax
import jax.numpy as jnp
from jax import lax
from jax.experimental import pallas as pl
from jax.experimental.pallas import tpu as pltpu
from jax.sharding import PartitionSpec as P

MESH = pl.DeviceIdType.MESH
DEV = 128
SLOTS = 4
CHUNKS = 8
PER = DEV // CHUNKS
FCH = 8


def position():
    z = lax.axis_index("gx")
    g = lax.axis_index("gy")
    y = lax.div(g, 8)
    x = lax.rem(lax.div(g, 2), 4)
    c = lax.rem(g, 2)
    return z, y, x, c


def peer(me, step, sign):
    z, y, x, c = me
    mixed = lax.rem(step * 37, DEV)
    oc = lax.rem(mixed, 2)
    ox = lax.rem(lax.div(mixed, 2), 4)
    oy = lax.rem(lax.div(mixed, 8), 4)
    oz = lax.div(mixed, 32)
    z2 = lax.rem(z + 4 + sign * oz, 4)
    y2 = lax.rem(y + 4 + sign * oy, 4)
    x2 = lax.rem(x + 4 + sign * ox, 4)
    c2 = lax.rem(c + oc, 2)
    return z2, y2 * 8 + x2 * 2 + c2


def exchange_kernel(
    src_s, tgt_s, blk_s, val_s, rad, area, f_hbm,
    fwd_out, bwd_in, idx_in,
    fv, wtd, sbwd, srad, rrad, sidx, idx_s,
    fsem, isem, idx_send, idx_recv, bwd_send, bwd_recv, rad_send, rad_recv,
):
    me = position()

    def f_copy(i):
        rows = pl.ds(i * (512 // FCH), 512 // FCH)
        return pltpu.make_async_copy(f_hbm.at[rows], fv.at[rows], fsem.at[i])

    for i in range(FCH):
        f_copy(i).start()

    barrier = pltpu.get_barrier_semaphore()

    @pl.loop(1, DEV)
    def _(s):
        pl.semaphore_signal(barrier, inc=1, device_id=peer(me, s, 1), device_id_type=MESH)

    lane = lax.broadcasted_iota(jnp.int32, (1, 128), 1)

    def index_row(s):
        z2, g2 = peer(me, s, 1)
        p = z2 * 32 + g2
        live = val_s[0, p]
        row = jnp.zeros((1, 128), jnp.int32)
        for k in range(SLOTS):
            q = src_s[0, p * SLOTS + k]
            q = jnp.where(k < live, q, q + 64)
            row = jnp.where(lane == k, q, row)
        return row

    idx_in[0] = index_row(0)

    @pl.loop(1, DEV)
    def _(s):
        sidx[s] = index_row(s)

    @pl.loop(0, 64)
    def _(c):
        wtd[c] = (area[pl.ds(c, 1), :] * rad[c].astype(jnp.float32)).astype(jnp.bfloat16)

    pl.semaphore_wait(barrier, DEV - 1)

    def idx_copy(s):
        return pltpu.make_async_remote_copy(
            src_ref=sidx.at[s], dst_ref=idx_in.at[s], send_sem=idx_send, recv_sem=idx_recv,
            device_id=peer(me, s, 1), device_id_type=MESH,
        )

    @pl.loop(1, DEV)
    def _(s):
        idx_copy(s).start()

    for i in range(FCH):
        f_copy(i).wait()

    def bwd_copy(s):
        return pltpu.make_async_remote_copy(
            src_ref=sbwd.at[s], dst_ref=bwd_in.at[s], send_sem=bwd_send,
            recv_sem=bwd_recv, device_id=peer(me, s, 1), device_id_type=MESH,
        )

    def bwd_step(s, out):
        z2, g2 = peer(me, s, 1)
        base = (z2 * 32 + g2) * SLOTS
        for k in range(SLOTS):
            w = wtd[tgt_s[0, base + k]]
            f = fv[blk_s[0, base + k]]
            out[s, k] = jnp.dot(w, f, preferred_element_type=jnp.float32).astype(jnp.bfloat16)

    bwd_step(1, sbwd)

    @pl.loop(2, DEV)
    def _(s):
        bwd_step(s, sbwd)
        bwd_copy(s - 1).start()

    bwd_step(0, bwd_in)
    bwd_copy(DEV - 1).start()

    rest = pl.ds(1, DEV - 1)
    idx_all = pltpu.make_async_remote_copy(
        src_ref=sidx.at[rest], dst_ref=idx_in.at[rest], send_sem=idx_send, recv_sem=idx_recv,
        device_id=peer(me, 1, 1), device_id_type=MESH,
    )
    idx_all.wait()
    to_smem = pltpu.make_async_copy(idx_in, idx_s, isem)
    to_smem.start()
    to_smem.wait()

    def rad_copy(s):
        return pltpu.make_async_remote_copy(
            src_ref=srad.at[s], dst_ref=rrad.at[s], send_sem=rad_send,
            recv_sem=rad_recv.at[lax.div(s, PER)], device_id=peer(me, s, -1), device_id_type=MESH,
        )

    def rad_step(s, out):
        for k in range(SLOTS):
            out[s, k] = rad[lax.rem(idx_s[s, 0, k], 64)]

    rad_step(1, srad)

    @pl.loop(2, DEV)
    def _(s):
        rad_step(s, srad)
        rad_copy(s - 1).start()

    rad_step(0, rrad)
    rad_copy(DEV - 1).start()

    def fwd_step(s):
        z2, g2 = peer(me, s, 1)
        base = (z2 * 32 + g2) * SLOTS
        for k in range(SLOTS):
            f = fv[blk_s[0, base + k]]
            fwd_out[s, k] = lax.dot_general(
                rrad[s, k], f, (((1,), (1,)), ((), ())), preferred_element_type=jnp.float32
            )

    for c in range(CHUNKS):
        first = max(1, c * PER)
        rows = pl.ds(first, (c + 1) * PER - first)
        pltpu.make_async_remote_copy(
            src_ref=srad.at[rows], dst_ref=rrad.at[rows], send_sem=rad_send,
            recv_sem=rad_recv.at[c], device_id=peer(me, 1, -1), device_id_type=MESH,
        ).wait_recv()

        @pl.loop(c * PER, (c + 1) * PER)
        def _(s):
            fwd_step(s)

    bwd_all = pltpu.make_async_remote_copy(
        src_ref=sbwd.at[rest], dst_ref=bwd_in.at[rest], send_sem=bwd_send, recv_sem=bwd_recv,
        device_id=peer(me, 1, 1), device_id_type=MESH,
    )
    bwd_all.wait()
    pltpu.make_async_remote_copy(
        src_ref=srad.at[rest], dst_ref=rrad.at[rest], send_sem=rad_send, recv_sem=rad_recv.at[0],
        device_id=peer(me, 1, -1), device_id_type=MESH,
    ).wait_send()


def combine_kernel(
    tgt_s, val_s, idx_s, fwd, bwd, area, emission, reflectance, out, gat, ret
):
    me = position()
    gat[...] = jnp.zeros_like(gat)
    ret[...] = jnp.zeros_like(ret)

    @pl.loop(0, DEV)
    def _(s):
        z2, g2 = peer(me, s, 1)
        p = z2 * 32 + g2
        live = val_s[0, p]
        for k in range(SLOTS):
            t = jnp.where(k < live, tgt_s[0, p * SLOTS + k], 64)
            q = jnp.minimum(idx_s[s, 0, k], 64)
            gat[t] += fwd[s, k]
            ret[q] += bwd[s, k].astype(jnp.float32)

    @pl.loop(0, 64)
    def _(c):
        irr = gat[c] + ret[c] / area[pl.ds(c, 1), :]
        out[c] = emission[c] + reflectance[c] * irr


def shards(
    radiance, emission, reflectance, patch_area, form_factor,
    source_index, target_index, block_index, valid_count,
):
    smem = pl.BlockSpec(memory_space=pltpu.SMEM)
    vmem = pl.BlockSpec(memory_space=pltpu.VMEM)
    hbm = pl.BlockSpec(memory_space=pl.ANY)
    slab = (DEV, SLOTS, 16, 128)
    dma = pltpu.SemaphoreType.DMA
    fwd, bwd, idx = pl.pallas_call(
        exchange_kernel,
        out_shape=(
            jax.ShapeDtypeStruct(slab, jnp.float32),
            jax.ShapeDtypeStruct(slab, jnp.bfloat16),
            jax.ShapeDtypeStruct((DEV, 1, 128), jnp.int32),
        ),
        in_specs=[smem, smem, smem, smem, vmem, vmem, hbm],
        out_specs=(vmem, vmem, vmem),
        scratch_shapes=[
            pltpu.VMEM((512, 128, 128), jnp.bfloat16),
            pltpu.VMEM((64, 16, 128), jnp.bfloat16),
            pltpu.VMEM(slab, jnp.bfloat16),
            pltpu.VMEM(slab, jnp.bfloat16),
            pltpu.VMEM(slab, jnp.bfloat16),
            pltpu.VMEM((DEV, 1, 128), jnp.int32),
            pltpu.SMEM((DEV, 1, 128), jnp.int32),
            dma((FCH,)), dma, dma, dma, dma, dma, dma, dma((CHUNKS,)),
        ],
        compiler_params=pltpu.CompilerParams(
            collective_id=0, has_side_effects=True, vmem_limit_bytes=48 << 20
        ),
        name="exchange",
    )(source_index, target_index, block_index, valid_count, radiance, patch_area, form_factor)
    return pl.pallas_call(
        combine_kernel,
        out_shape=jax.ShapeDtypeStruct((64, 16, 128), jnp.float32),
        in_specs=[smem, smem, smem, vmem, vmem, vmem, vmem, vmem],
        out_specs=vmem,
        scratch_shapes=[
            pltpu.VMEM((65, 16, 128), jnp.float32),
            pltpu.VMEM((65, 16, 128), jnp.float32),
        ],
        compiler_params=pltpu.CompilerParams(vmem_limit_bytes=24 << 20),
        name="combine",
    )(target_index, valid_count, idx, fwd, bwd, patch_area, emission, reflectance)


def solution(mesh):
    both = ("gx", "gy")
    in_specs = (
        P(both, None, None),
        P(both, None, None),
        P(both, None, None),
        P(both, None),
        P(both, None, None),
        P(both, None),
        P(both, None),
        P(both, None),
        P(both, None),
    )
    return jax.shard_map(
        shards, mesh=mesh, in_specs=in_specs, out_specs=P(both, None, None), check_vma=False
    )
```

```python
import jax
import jax.numpy as jnp
from jax import lax
from jax.experimental import pallas as pl
from jax.experimental.pallas import tpu as pltpu
from jax.sharding import PartitionSpec as P

MESH = pl.DeviceIdType.MESH
DEV = 128
SLOTS = 4
GROUPS = 32
GRP = DEV // GROUPS
EARLY = 8
CHUNKS = 4
PER = DEV // CHUNKS
FCH = 8
MIX = 59


def position():
    z = lax.axis_index("gx")
    g = lax.axis_index("gy")
    y = lax.div(g, 8)
    x = lax.rem(lax.div(g, 2), 4)
    c = lax.rem(g, 2)
    return z, y, x, c


def peer(me, step, sign):
    z, y, x, c = me
    mixed = lax.rem(step * MIX, DEV)
    oc = lax.rem(mixed, 2)
    ox = lax.rem(lax.div(mixed, 2), 4)
    oy = lax.rem(lax.div(mixed, 8), 4)
    oz = lax.div(mixed, 32)
    z2 = lax.rem(z + 4 + sign * oz, 4)
    y2 = lax.rem(y + 4 + sign * oy, 4)
    x2 = lax.rem(x + 4 + sign * ox, 4)
    c2 = lax.rem(c + oc, 2)
    return z2, y2 * 8 + x2 * 2 + c2


def exchange_kernel(
    src_h, tgt_h, blk_h, val_h, rad_h, area_h, f_h,
    irr,
    src_s, tgt_s, blk_s, val_s, rad, area,
    fv, wtd, sbwd, bwd_0, bwd_1, bwd_2, bwd_3, srad, rrad, fwd, sidx, idx_in, tidx, seq, gat, ret,
    meta_v, idx_s, meta_s,
    lsem, fsem, msem, idx_send, idx_recv, bwd_send, bwd_recv, rad_send, rad_recv,
):
    me = position()
    bwd_in = (bwd_0, bwd_1, bwd_2, bwd_3)

    loads = [
        pltpu.make_async_copy(a, b, lsem.at[i])
        for i, (a, b) in enumerate(
            [(src_h, src_s), (tgt_h, tgt_s), (blk_h, blk_s), (val_h, val_s), (rad_h, rad), (area_h, area)]
        )
    ]
    for load in loads:
        load.start()

    def f_copy(i):
        rows = pl.ds(i * (512 // FCH), 512 // FCH)
        return pltpu.make_async_copy(f_h.at[rows], fv.at[rows], fsem.at[i])

    for i in range(FCH):
        f_copy(i).start()

    barrier = pltpu.get_barrier_semaphore()

    @pl.loop(1, DEV)
    def _(s):
        pl.semaphore_signal(barrier, inc=1, device_id=peer(me, s, 1), device_id_type=MESH)

    for load in loads:
        load.wait()

    lane = lax.broadcasted_iota(jnp.int32, (1, 128), 1)

    @pl.loop(0, DEV)
    def _(s):
        z2, g2 = peer(me, s, 1)
        p = z2 * 32 + g2
        live = val_s[0, p]
        srow = jnp.zeros((1, 128), jnp.int32)
        trow = jnp.zeros((1, 128), jnp.int32)
        for k in range(SLOTS):
            dead = jnp.where(k < live, 0, 64)
            srow = jnp.where(lane == k, src_s[0, p * SLOTS + k] + dead, srow)
            trow = jnp.where(lane == k, tgt_s[0, p * SLOTS + k] + dead, trow)
        sidx[s] = srow
        tidx[s] = trow

    idx_in[0] = sidx[0]

    @pl.loop(0, 64)
    def _(c):
        wtd[c] = (area[pl.ds(c, 1), :] * rad[c].astype(jnp.float32)).astype(jnp.bfloat16)

    pl.semaphore_wait(barrier, DEV - 1)

    def idx_copy(rows, s):
        return pltpu.make_async_remote_copy(
            src_ref=sidx.at[rows], dst_ref=idx_in.at[rows], send_sem=idx_send, recv_sem=idx_recv,
            device_id=peer(me, s, 1), device_id_type=MESH,
        )

    @pl.loop(1, DEV)
    def _(s):
        idx_copy(s, s).start()

    def bwd_copy(first, count, s, c):
        return pltpu.make_async_remote_copy(
            src_ref=sbwd.at[pl.ds(first, count)],
            dst_ref=bwd_in[c].at[pl.ds(first - c * PER, count)],
            send_sem=bwd_send.at[c], recv_sem=bwd_recv.at[c],
            device_id=peer(me, s, 1), device_id_type=MESH,
        )

    def bwd_rest(c):
        first = max(1, c * PER)
        return bwd_copy(first, (c + 1) * PER - first, 1, c)

    def rad_copy(rows, s, c):
        return pltpu.make_async_remote_copy(
            src_ref=srad.at[rows], dst_ref=rrad.at[rows], send_sem=rad_send,
            recv_sem=rad_recv.at[c], device_id=peer(me, s, -1), device_id_type=MESH,
        )

    def send_rad(g, first=0):
        for j in range(first, GRP):
            s = g * GRP + j
            rad_copy(s, s, lax.div(s, PER)).start()

    def send_bwd(g, c, first=0):
        for j in range(first, GRP):
            s = g * GRP + j
            bwd_copy(s, 1, s, c).start()

    def bwd_group(g):
        for j in range(GRP):
            s = g * GRP + j
            z2, g2 = peer(me, s, 1)
            base = (z2 * 32 + g2) * SLOTS
            for k in range(0, SLOTS, 2):
                w = jnp.concatenate([wtd[tgt_s[0, base + k]], wtd[tgt_s[0, base + k + 1]]], axis=0)
                f = jnp.concatenate([fv[blk_s[0, base + k]], fv[blk_s[0, base + k + 1]]], axis=1)
                r = jnp.dot(w, f, preferred_element_type=jnp.float32)
                sbwd[s, k] = r[:16, :128].astype(jnp.bfloat16)
                sbwd[s, k + 1] = r[16:, 128:].astype(jnp.bfloat16)

    def fwd_group(g):
        for j in range(GRP):
            s = g * GRP + j
            z2, g2 = peer(me, s, 1)
            base = (z2 * 32 + g2) * SLOTS
            for k in range(0, SLOTS, 2):
                v = jnp.concatenate([rrad[s, k], rrad[s, k + 1]], axis=0)
                f = jnp.concatenate([fv[blk_s[0, base + k]], fv[blk_s[0, base + k + 1]]], axis=0)
                r = lax.dot_general(v, f, (((1,), (1,)), ((), ())), preferred_element_type=jnp.float32)
                fwd[s, k] = r[:16, :128]
                fwd[s, k + 1] = r[16:, 128:]

    for i in range(FCH):
        f_copy(i).wait()

    bwd_group(0)
    bwd_group(1)
    send_bwd(0, 0, 1)

    @pl.loop(2, EARLY + 1)
    def _(g):
        bwd_group(g)
        send_bwd(g - 1, 0)

    @pl.loop(EARLY + 1, GROUPS)
    def _(g):
        bwd_group(g)

    for k in range(SLOTS):
        bwd_0[0, k] = sbwd[0, k]

    rest = pl.ds(1, DEV - 1)
    idx_copy(rest, 1).wait()
    to_smem = pltpu.make_async_copy(idx_in, idx_s, msem.at[0])
    to_smem.start()
    to_smem.wait()

    def rad_group(g):
        for j in range(GRP):
            s = g * GRP + j
            for k in range(SLOTS):
                srad[s, k] = rad[lax.rem(idx_s[s, 0, k], 64)]

    rad_group(0)
    rad_group(1)
    send_rad(0, 1)

    @pl.loop(2, GROUPS)
    def _(g):
        rad_group(g)
        send_rad(g - 1)

    for k in range(SLOTS):
        rrad[0, k] = srad[0, k]
    send_rad(GROUPS - 1)

    for c in range(EARLY // (GROUPS // CHUNKS), CHUNKS):

        @pl.loop(c * (GROUPS // CHUNKS), (c + 1) * (GROUPS // CHUNKS))
        def _(g):
            send_bwd(g, c)

    def order(ids, c, base):
        block = ids[pl.ds(c * PER, PER)].reshape(PER, 128)
        q = jnp.concatenate(
            [jnp.broadcast_to(block[:, k : k + 1], (PER, 128)) for k in range(SLOTS)], axis=0
        )
        lanes = lax.broadcasted_iota(jnp.int32, (128, 128), 1)
        key = q * 128 + lax.broadcasted_iota(jnp.int32, (128, 128), 0)
        rank = jnp.sum((key.T < key).astype(jnp.int32), axis=1, keepdims=True)
        meta_v[base + 2 * c] = jnp.sum(jnp.where(rank == lanes, key, 0), axis=0, keepdims=True)
        upto = jnp.sum((q <= lanes).astype(jnp.int32), axis=0, keepdims=True)
        below = jnp.sum((q < lanes).astype(jnp.int32), axis=0, keepdims=True)
        meta_v[base + 2 * c + 1] = jnp.where(upto > below, upto, 0)

    @pl.loop(0, CHUNKS)
    def _(c):
        order(tidx, c, 0)
        order(idx_in, c, 2 * CHUNKS)

    to_smem = pltpu.make_async_copy(meta_v, meta_s, msem.at[1])
    to_smem.start()
    to_smem.wait()

    seq[0] = jnp.zeros((16, 128), jnp.float32)
    gat[...] = jnp.zeros_like(gat)
    ret[...] = jnp.zeros_like(ret)

    def scan(values, offset, total, c, base):
        def body(i, carry):
            acc, last = carry
            for j in range(8):
                n = i * 8 + j
                key = meta_s[base + 2 * c, 0, n]
                q = lax.div(key, 128)
                item = lax.rem(key, 128)
                x = values[offset + lax.rem(item, PER), lax.div(item, PER)].astype(jnp.float32)
                acc = acc * jnp.where(q == last, 1.0, 0.0) + x
                seq[n + 1] = acc
                last = q
            return acc, last

        lax.fori_loop(0, 16, body, (jnp.zeros((16, 128), jnp.float32), jnp.int32(-1)))

        @pl.loop(0, 16)
        def _(i):
            for j in range(4):
                t = i * 4 + j
                total[t] += seq[meta_s[base + 2 * c + 1, 0, t]]

    for c in range(CHUNKS):
        first = max(1, c * PER)
        rad_copy(pl.ds(first, (c + 1) * PER - first), 1, c).wait_recv()

        @pl.loop(c * (GROUPS // CHUNKS), (c + 1) * (GROUPS // CHUNKS))
        def _(g):
            fwd_group(g)

        scan(fwd, c * PER, gat, c, 0)

    for c in range(CHUNKS):
        bwd_rest(c).wait_recv()
        scan(bwd_in[c], 0, ret, c, 2 * CHUNKS)

    @pl.loop(0, 64)
    def _(c):
        irr[c] = gat[c] + ret[c] / area[pl.ds(c, 1), :]

    for c in range(CHUNKS):
        bwd_rest(c).wait_send()
    rad_copy(rest, 1, 0).wait_send()


def shards(
    radiance, emission, reflectance, patch_area, form_factor,
    source_index, target_index, block_index, valid_count,
):
    hbm = pl.BlockSpec(memory_space=pltpu.HBM)
    vmem = pl.BlockSpec(memory_space=pltpu.VMEM)
    slab = (DEV, SLOTS, 16, 128)
    rows = (DEV, 1, 128)
    dma = pltpu.SemaphoreType.DMA
    irr = pl.pallas_call(
        exchange_kernel,
        out_shape=jax.ShapeDtypeStruct((64, 16, 128), jnp.float32),
        in_specs=[hbm] * 7,
        out_specs=vmem,
        scratch_shapes=[
            pltpu.SMEM((1, 512), jnp.int32),
            pltpu.SMEM((1, 512), jnp.int32),
            pltpu.SMEM((1, 512), jnp.int32),
            pltpu.SMEM((1, 128), jnp.int32),
            pltpu.VMEM((64, 16, 128), jnp.bfloat16),
            pltpu.VMEM((64, 128), jnp.float32),
            pltpu.VMEM((512, 128, 128), jnp.bfloat16),
            pltpu.VMEM((64, 16, 128), jnp.bfloat16),
            pltpu.VMEM(slab, jnp.bfloat16),
            *[pltpu.VMEM((PER, SLOTS, 16, 128), jnp.bfloat16) for _ in range(CHUNKS)],
            pltpu.VMEM(slab, jnp.bfloat16),
            pltpu.VMEM(slab, jnp.bfloat16),
            pltpu.VMEM(slab, jnp.float32),
            pltpu.VMEM(rows, jnp.int32),
            pltpu.VMEM(rows, jnp.int32),
            pltpu.VMEM(rows, jnp.int32),
            pltpu.VMEM((136, 16, 128), jnp.float32),
            pltpu.VMEM((64, 16, 128), jnp.float32),
            pltpu.VMEM((64, 16, 128), jnp.float32),
            pltpu.VMEM((4 * CHUNKS, 1, 128), jnp.int32),
            pltpu.SMEM(rows, jnp.int32),
            pltpu.SMEM((4 * CHUNKS, 1, 128), jnp.int32),
            dma((6,)), dma((FCH,)), dma((2,)), dma, dma, dma((CHUNKS,)), dma((CHUNKS,)), dma, dma((CHUNKS,)),
        ],
        compiler_params=pltpu.CompilerParams(
            collective_id=0, has_side_effects=True, vmem_limit_bytes=67043328
        ),
        name="exchange",
    )(
        source_index, target_index, block_index, valid_count, radiance, patch_area, form_factor
    )
    return emission + reflectance * irr


def solution(mesh):
    both = ("gx", "gy")
    in_specs = (
        P(both, None, None),
        P(both, None, None),
        P(both, None, None),
        P(both, None),
        P(both, None, None),
        P(both, None),
        P(both, None),
        P(both, None),
        P(both, None),
    )
    return jax.shard_map(
        shards, mesh=mesh, in_specs=in_specs, out_specs=P(both, None, None), check_vma=False
    )
```

```python
import jax
import jax.numpy as jnp
from jax import lax
from jax.experimental import pallas as pl
from jax.experimental.pallas import tpu as pltpu
from jax.sharding import PartitionSpec as P

MESH = pl.DeviceIdType.MESH
DEV = 128
SLOTS = 4
GROUPS = 32
GRP = DEV // GROUPS
EARLY = 2
CHUNKS = 4
PER = DEV // CHUNKS
FCH = 8
MIX = 37


def position():
    z = lax.axis_index("gx")
    g = lax.axis_index("gy")
    y = lax.div(g, 8)
    x = lax.rem(lax.div(g, 2), 4)
    c = lax.rem(g, 2)
    return z, y, x, c


def peer(me, step, sign):
    z, y, x, c = me
    mixed = lax.rem(step * MIX, DEV)
    oc = lax.rem(mixed, 2)
    ox = lax.rem(lax.div(mixed, 2), 4)
    oy = lax.rem(lax.div(mixed, 8), 4)
    oz = lax.div(mixed, 32)
    z2 = lax.rem(z + 4 + sign * oz, 4)
    y2 = lax.rem(y + 4 + sign * oy, 4)
    x2 = lax.rem(x + 4 + sign * ox, 4)
    c2 = lax.rem(c + oc, 2)
    return z2, y2 * 8 + x2 * 2 + c2


def exchange_kernel(
    src_h, tgt_h, blk_h, val_h, rad_h, area_h, f_h,
    irr,
    src_s, tgt_s, blk_s, val_s, rad, area,
    fv, wtd, sbwd, bwd_0, bwd_1, bwd_2, bwd_3, srad, rrad, fwd, sidx, idx_in, tidx, seq, gat, ret,
    meta_v, idx_s, meta_s,
    lsem, fsem, msem, idx_send, idx_recv, bwd_send, bwd_recv, rad_send, rad_recv,
):
    me = position()
    bwd_in = (bwd_0, bwd_1, bwd_2, bwd_3)

    loads = [
        pltpu.make_async_copy(a, b, lsem.at[i])
        for i, (a, b) in enumerate(
            [(src_h, src_s), (tgt_h, tgt_s), (blk_h, blk_s), (val_h, val_s), (rad_h, rad), (area_h, area)]
        )
    ]
    for load in loads:
        load.start()

    def f_copy(i):
        rows = pl.ds(i * (512 // FCH), 512 // FCH)
        return pltpu.make_async_copy(f_h.at[rows], fv.at[rows], fsem.at[i])

    for i in range(FCH):
        f_copy(i).start()

    barrier = pltpu.get_barrier_semaphore()

    def by_peer(step):
        for s in range(1, GRP):
            step(s)

        @pl.loop(1, GROUPS)
        def _(g):
            for j in range(GRP):
                step(g * GRP + j)

    by_peer(
        lambda s: pl.semaphore_signal(barrier, inc=1, device_id=peer(me, s, 1), device_id_type=MESH)
    )

    for load in loads:
        load.wait()

    lane = lax.broadcasted_iota(jnp.int32, (1, 128), 1)

    def fill(rows, table):
        @pl.loop(0, GROUPS)
        def _(g):
            for j in range(GRP):
                s = g * GRP + j
                z2, g2 = peer(me, s, 1)
                p = z2 * 32 + g2
                live = val_s[0, p]
                row = jnp.zeros((1, 128), jnp.int32)
                for k in range(SLOTS):
                    row = jnp.where(lane == k, table[0, p * SLOTS + k] + jnp.where(k < live, 0, 64), row)
                rows[s] = row

    fill(sidx, src_s)
    idx_in[0] = sidx[0]

    pl.semaphore_wait(barrier, DEV - 1)

    def idx_copy(rows, s):
        return pltpu.make_async_remote_copy(
            src_ref=sidx.at[rows], dst_ref=idx_in.at[rows], send_sem=idx_send, recv_sem=idx_recv,
            device_id=peer(me, s, 1), device_id_type=MESH,
        )

    by_peer(lambda s: idx_copy(s, s).start())

    @pl.loop(0, 16)
    def _(i):
        for j in range(4):
            c = i * 4 + j
            wtd[c] = (area[pl.ds(c, 1), :] * rad[c].astype(jnp.float32)).astype(jnp.bfloat16)

    def bwd_copy(first, count, s, c):
        return pltpu.make_async_remote_copy(
            src_ref=sbwd.at[pl.ds(first, count)],
            dst_ref=bwd_in[c].at[pl.ds(first - c * PER, count)],
            send_sem=bwd_send.at[c], recv_sem=bwd_recv.at[c],
            device_id=peer(me, s, 1), device_id_type=MESH,
        )

    def bwd_rest(c):
        first = max(1, c * PER)
        return bwd_copy(first, (c + 1) * PER - first, 1, c)

    def rad_copy(rows, s, c):
        return pltpu.make_async_remote_copy(
            src_ref=srad.at[rows], dst_ref=rrad.at[rows], send_sem=rad_send,
            recv_sem=rad_recv.at[c], device_id=peer(me, s, -1), device_id_type=MESH,
        )

    def send_rad(g, first=0):
        for j in range(first, GRP):
            s = g * GRP + j
            rad_copy(s, s, lax.div(s, PER)).start()

    def send_bwd(g, c, first=0):
        for j in range(first, GRP):
            s = g * GRP + j
            bwd_copy(s, 1, s, c).start()

    def bwd_group(g):
        for j in range(GRP):
            s = g * GRP + j
            z2, g2 = peer(me, s, 1)
            base = (z2 * 32 + g2) * SLOTS
            for k in range(0, SLOTS, 2):
                w = jnp.concatenate([wtd[tgt_s[0, base + k]], wtd[tgt_s[0, base + k + 1]]], axis=0)
                f = jnp.concatenate([fv[blk_s[0, base + k]], fv[blk_s[0, base + k + 1]]], axis=1)
                r = jnp.dot(w, f, preferred_element_type=jnp.float32)
                sbwd[s, k] = r[:16, :128].astype(jnp.bfloat16)
                sbwd[s, k + 1] = r[16:, 128:].astype(jnp.bfloat16)

    def fwd_group(g):
        for j in range(GRP):
            s = g * GRP + j
            z2, g2 = peer(me, s, 1)
            base = (z2 * 32 + g2) * SLOTS
            for k in range(0, SLOTS, 2):
                v = jnp.concatenate([rrad[s, k], rrad[s, k + 1]], axis=0)
                f = jnp.concatenate([fv[blk_s[0, base + k]], fv[blk_s[0, base + k + 1]]], axis=0)
                r = lax.dot_general(v, f, (((1,), (1,)), ((), ())), preferred_element_type=jnp.float32)
                fwd[s, k] = r[:16, :128]
                fwd[s, k + 1] = r[16:, 128:]

    for i in range(FCH):
        f_copy(i).wait()

    bwd_group(0)
    bwd_group(1)
    send_bwd(0, 0, 1)

    lap = GROUPS // CHUNKS

    @pl.loop(2, lap + 1)
    def _(g):
        bwd_group(g)
        send_bwd(g - 1, 0)

    for c in range(1, EARLY):

        @pl.loop(c * lap + 1, (c + 1) * lap + 1)
        def _(g):
            bwd_group(g)
            send_bwd(g - 1, c)

    @pl.loop(EARLY * lap + 1, GROUPS)
    def _(g):
        bwd_group(g)

    fill(tidx, tgt_s)

    for k in range(SLOTS):
        bwd_0[0, k] = sbwd[0, k]

    rest = pl.ds(1, DEV - 1)
    idx_copy(rest, 1).wait()
    to_smem = pltpu.make_async_copy(idx_in, idx_s, msem.at[0])
    to_smem.start()
    to_smem.wait()

    def rad_group(g):
        for j in range(GRP):
            s = g * GRP + j
            for k in range(SLOTS):
                srad[s, k] = rad[lax.rem(idx_s[s, 0, k], 64)]

    rad_group(0)
    rad_group(1)
    send_rad(0, 1)

    @pl.loop(2, GROUPS)
    def _(g):
        rad_group(g)
        send_rad(g - 1)

    for k in range(SLOTS):
        rrad[0, k] = srad[0, k]
    send_rad(GROUPS - 1)

    for c in range(EARLY, CHUNKS):

        @pl.loop(c * lap, (c + 1) * lap)
        def _(g):
            send_bwd(g, c)

    def order(ids, c, base):
        block = ids[pl.ds(c * PER, PER)].reshape(PER, 128)
        q = jnp.concatenate(
            [jnp.broadcast_to(block[:, k : k + 1], (PER, 128)) for k in range(SLOTS)], axis=0
        )
        lanes = lax.broadcasted_iota(jnp.int32, (128, 128), 1)
        key = q * 128 + lax.broadcasted_iota(jnp.int32, (128, 128), 0)
        rank = jnp.sum((key.T < key).astype(jnp.int32), axis=1, keepdims=True)
        meta_v[base + 2 * c] = jnp.sum(jnp.where(rank == lanes, key, 0), axis=0, keepdims=True)
        upto = jnp.sum((q <= lanes).astype(jnp.int32), axis=0, keepdims=True)
        below = jnp.sum((q < lanes).astype(jnp.int32), axis=0, keepdims=True)
        meta_v[base + 2 * c + 1] = jnp.where(upto > below, upto, 0)

    @pl.loop(0, CHUNKS)
    def _(c):
        order(tidx, c, 0)
        order(idx_in, c, 2 * CHUNKS)

    to_smem = pltpu.make_async_copy(meta_v, meta_s, msem.at[1])
    to_smem.start()
    to_smem.wait()

    seq[0] = jnp.zeros((16, 128), jnp.float32)
    gat[...] = jnp.zeros_like(gat)
    ret[...] = jnp.zeros_like(ret)

    def scan(values, offset, total, c, base):
        def body(i, carry):
            acc, last = carry
            for j in range(8):
                n = i * 8 + j
                key = meta_s[base + 2 * c, 0, n]
                q = lax.div(key, 128)
                item = lax.rem(key, 128)
                x = values[offset + lax.rem(item, PER), lax.div(item, PER)].astype(jnp.float32)
                acc = acc * jnp.where(q == last, 1.0, 0.0) + x
                seq[n + 1] = acc
                last = q
            return acc, last

        lax.fori_loop(0, 16, body, (jnp.zeros((16, 128), jnp.float32), jnp.int32(-1)))

        @pl.loop(0, 16)
        def _(i):
            for j in range(4):
                t = i * 4 + j
                total[t] += seq[meta_s[base + 2 * c + 1, 0, t]]

    for c in range(CHUNKS):
        first = max(1, c * PER)
        rad_copy(pl.ds(first, (c + 1) * PER - first), 1, c).wait_recv()

        @pl.loop(c * lap, (c + 1) * lap)
        def _(g):
            fwd_group(g)

        scan(fwd, c * PER, gat, c, 0)

    for c in range(CHUNKS):
        bwd_rest(c).wait_recv()
        scan(bwd_in[c], 0, ret, c, 2 * CHUNKS)

    @pl.loop(0, 64)
    def _(c):
        irr[c] = gat[c] + ret[c] / area[pl.ds(c, 1), :]

    for c in range(CHUNKS):
        bwd_rest(c).wait_send()
    rad_copy(rest, 1, 0).wait_send()


def shards(
    radiance, emission, reflectance, patch_area, form_factor,
    source_index, target_index, block_index, valid_count,
):
    hbm = pl.BlockSpec(memory_space=pltpu.HBM)
    vmem = pl.BlockSpec(memory_space=pltpu.VMEM)
    slab = (DEV, SLOTS, 16, 128)
    rows = (DEV, 1, 128)
    dma = pltpu.SemaphoreType.DMA
    irr = pl.pallas_call(
        exchange_kernel,
        out_shape=jax.ShapeDtypeStruct((64, 16, 128), jnp.float32),
        in_specs=[hbm] * 7,
        out_specs=vmem,
        scratch_shapes=[
            pltpu.SMEM((1, 512), jnp.int32),
            pltpu.SMEM((1, 512), jnp.int32),
            pltpu.SMEM((1, 512), jnp.int32),
            pltpu.SMEM((1, 128), jnp.int32),
            pltpu.VMEM((64, 16, 128), jnp.bfloat16),
            pltpu.VMEM((64, 128), jnp.float32),
            pltpu.VMEM((512, 128, 128), jnp.bfloat16),
            pltpu.VMEM((64, 16, 128), jnp.bfloat16),
            pltpu.VMEM(slab, jnp.bfloat16),
            *[pltpu.VMEM((PER, SLOTS, 16, 128), jnp.bfloat16) for _ in range(CHUNKS)],
            pltpu.VMEM(slab, jnp.bfloat16),
            pltpu.VMEM(slab, jnp.bfloat16),
            pltpu.VMEM(slab, jnp.float32),
            pltpu.VMEM(rows, jnp.int32),
            pltpu.VMEM(rows, jnp.int32),
            pltpu.VMEM(rows, jnp.int32),
            pltpu.VMEM((136, 16, 128), jnp.float32),
            pltpu.VMEM((64, 16, 128), jnp.float32),
            pltpu.VMEM((64, 16, 128), jnp.float32),
            pltpu.VMEM((4 * CHUNKS, 1, 128), jnp.int32),
            pltpu.SMEM(rows, jnp.int32),
            pltpu.SMEM((4 * CHUNKS, 1, 128), jnp.int32),
            dma((6,)), dma((FCH,)), dma((2,)), dma, dma, dma((CHUNKS,)), dma((CHUNKS,)), dma, dma((CHUNKS,)),
        ],
        compiler_params=pltpu.CompilerParams(
            collective_id=0, has_side_effects=True, vmem_limit_bytes=48 << 20
        ),
        name="exchange",
    )(
        *[pltpu.with_memory_space_constraint(v, pltpu.HBM) for v in (source_index, target_index, block_index, valid_count, radiance, patch_area, form_factor)]
    )
    return emission + reflectance * irr


def solution(mesh):
    both = ("gx", "gy")
    in_specs = (
        P(both, None, None),
        P(both, None, None),
        P(both, None, None),
        P(both, None),
        P(both, None, None),
        P(both, None),
        P(both, None),
        P(both, None),
        P(both, None),
    )
    return jax.shard_map(
        shards, mesh=mesh, in_specs=in_specs, out_specs=P(both, None, None), check_vma=False
    )
```

```python
import jax
import jax.numpy as jnp
from jax import lax
from jax.experimental import pallas as pl
from jax.experimental.pallas import tpu as pltpu
from jax.sharding import PartitionSpec as P

MESH = pl.DeviceIdType.MESH
DEV = 128
SLOTS = 4
GROUPS = 32
GRP = DEV // GROUPS
EARLY = 2
CHUNKS = 4
PER = DEV // CHUNKS
FCH = 8
MIX = 13


def position():
    z = lax.axis_index("gx")
    g = lax.axis_index("gy")
    y = lax.div(g, 8)
    x = lax.rem(lax.div(g, 2), 4)
    c = lax.rem(g, 2)
    return z, y, x, c


def peer(me, step, sign):
    z, y, x, c = me
    mixed = lax.rem(step * MIX, DEV)
    oc = lax.rem(mixed, 2)
    ox = lax.rem(lax.div(mixed, 2), 4)
    oy = lax.rem(lax.div(mixed, 8), 4)
    oz = lax.div(mixed, 32)
    z2 = lax.rem(z + 4 + sign * oz, 4)
    y2 = lax.rem(y + 4 + sign * oy, 4)
    x2 = lax.rem(x + 4 + sign * ox, 4)
    c2 = lax.rem(c + oc, 2)
    return z2, y2 * 8 + x2 * 2 + c2


def index_spot(step):
    mixed = lax.rem(step * MIX, DEV)
    return lax.rem(mixed, 2), lax.div(mixed, 2)


def chip(me, m):
    z, y, x, _ = me
    return (
        lax.rem(z + lax.div(m, 16), 4),
        lax.rem(y + lax.rem(lax.div(m, 4), 4), 4) * 8 + lax.rem(x + lax.rem(m, 4), 4) * 2,
    )


def exchange_kernel(
    src_h, tgt_h, blk_h, val_h, rad_h, area_h, f_h,
    irr,
    src_s, tgt_s, blk_s, val_s, rad, area,
    fv, wtd, sbwd, bwd_0, bwd_1, bwd_2, bwd_3, srad, rrad, fwd, sidx, idx_in, tidx, ridx, seq, gat, ret,
    meta_v, meta_s,
    lsem, fsem, msem, idx_send, idx_recv, pair_send, pair_recv, bwd_send, bwd_recv, rad_send, rad_recv,
):
    me = position()
    bwd_in = (bwd_0, bwd_1, bwd_2, bwd_3)

    loads = [
        pltpu.make_async_copy(a, b, lsem.at[i])
        for i, (a, b) in enumerate(
            [(src_h, src_s), (tgt_h, tgt_s), (blk_h, blk_s), (val_h, val_s), (rad_h, rad), (area_h, area)]
        )
    ]
    for load in loads:
        load.start()

    def f_copy(i):
        rows = pl.ds(i * (512 // FCH), 512 // FCH)
        return pltpu.make_async_copy(f_h.at[rows], fv.at[rows], fsem.at[i])

    for i in range(FCH):
        f_copy(i).start()

    barrier = pltpu.get_barrier_semaphore()

    def by_peer(step):
        for s in range(1, GRP):
            step(s)

        @pl.loop(1, GROUPS)
        def _(g):
            for j in range(GRP):
                step(g * GRP + j)

    by_peer(
        lambda s: pl.semaphore_signal(barrier, inc=1, device_id=peer(me, s, 1), device_id_type=MESH)
    )

    for load in loads:
        load.wait()

    lane = lax.broadcasted_iota(jnp.int32, (1, 128), 1)

    def fill(rows, table):
        @pl.loop(0, GROUPS)
        def _(g):
            for j in range(GRP):
                s = g * GRP + j
                z2, g2 = peer(me, s, 1)
                p = z2 * 32 + g2
                live = val_s[0, p]
                row = jnp.zeros((1, 128), jnp.int32)
                for k in range(SLOTS):
                    row = jnp.where(lane == k, table[0, p * SLOTS + k] + jnp.where(k < live, 0, 64), row)
                rows[s] = row

    @pl.loop(0, 32)
    def _(i):
        for j in range(2):
            m = i * 2 + j
            z2, g2 = chip(me, m)
            row = jnp.zeros((1, 128), jnp.int32)
            for c in range(2):
                p = z2 * 32 + g2 + c
                live = val_s[0, p]
                for k in range(SLOTS):
                    q = src_s[0, p * SLOTS + k] + jnp.where(k < live, 0, 64)
                    row = jnp.where(lane == c * SLOTS + k, q, row)
            sidx[m] = row

    idx_in[0, 0] = sidx[0]

    @pl.loop(0, 16)
    def _(i):
        for j in range(4):
            c = i * 4 + j
            wtd[c] = (area[pl.ds(c, 1), :] * rad[c].astype(jnp.float32)).astype(jnp.bfloat16)

    pl.semaphore_wait(barrier, DEV - 1)

    core = me[3]

    def idx_copy(rows, m):
        z2, g2 = chip(me, m)
        return pltpu.make_async_remote_copy(
            src_ref=sidx.at[rows], dst_ref=idx_in.at[0, rows], send_sem=idx_send, recv_sem=idx_recv,
            device_id=(z2, g2 + core), device_id_type=MESH,
        )

    def pair_copy():
        z2, g2 = chip(me, 0)
        return pltpu.make_async_remote_copy(
            src_ref=idx_in.at[0], dst_ref=idx_in.at[1], send_sem=pair_send, recv_sem=pair_recv,
            device_id=(z2, g2 + 1 - core), device_id_type=MESH,
        )

    for m in range(1, 3):
        idx_copy(m, m).start()

    @pl.loop(1, 21)
    def _(i):
        for j in range(3):
            m = i * 3 + j
            idx_copy(m, m).start()

    idx_copy(63, 63).start()

    def bwd_copy(first, count, s, c):
        return pltpu.make_async_remote_copy(
            src_ref=sbwd.at[pl.ds(first, count)],
            dst_ref=bwd_in[c].at[pl.ds(first - c * PER, count)],
            send_sem=bwd_send.at[c], recv_sem=bwd_recv.at[c],
            device_id=peer(me, s, 1), device_id_type=MESH,
        )

    def bwd_rest(c):
        first = max(1, c * PER)
        return bwd_copy(first, (c + 1) * PER - first, 1, c)

    def rad_copy(rows, s, c):
        return pltpu.make_async_remote_copy(
            src_ref=srad.at[rows], dst_ref=rrad.at[rows], send_sem=rad_send.at[c],
            recv_sem=rad_recv.at[c], device_id=peer(me, s, -1), device_id_type=MESH,
        )

    def rad_rest(c):
        first = max(1, c * PER)
        return rad_copy(pl.ds(first, (c + 1) * PER - first), 1, c)

    def send_rad(g, c, first=0):
        for j in range(first, GRP):
            s = g * GRP + j
            rad_copy(s, s, c).start()

    def send_bwd(g, c, first=0):
        for j in range(first, GRP):
            s = g * GRP + j
            bwd_copy(s, 1, s, c).start()

    def bwd_group(g):
        for j in range(GRP):
            s = g * GRP + j
            z2, g2 = peer(me, s, 1)
            base = (z2 * 32 + g2) * SLOTS
            for k in range(0, SLOTS, 2):
                w = jnp.concatenate([wtd[tgt_s[0, base + k]], wtd[tgt_s[0, base + k + 1]]], axis=0)
                f = jnp.concatenate([fv[blk_s[0, base + k]], fv[blk_s[0, base + k + 1]]], axis=1)
                r = jnp.dot(w, f, preferred_element_type=jnp.float32)
                sbwd[s, k] = r[:16, :128].astype(jnp.bfloat16)
                sbwd[s, k + 1] = r[16:, 128:].astype(jnp.bfloat16)

    def fwd_group(g):
        for j in range(GRP):
            s = g * GRP + j
            z2, g2 = peer(me, s, 1)
            base = (z2 * 32 + g2) * SLOTS
            for k in range(0, SLOTS, 2):
                v = jnp.concatenate([rrad[s, k], rrad[s, k + 1]], axis=0)
                f = jnp.concatenate([fv[blk_s[0, base + k]], fv[blk_s[0, base + k + 1]]], axis=0)
                r = lax.dot_general(v, f, (((1,), (1,)), ((), ())), preferred_element_type=jnp.float32)
                fwd[s, k] = r[:16, :128]
                fwd[s, k + 1] = r[16:, 128:]

    for i in range(FCH):
        f_copy(i).wait()

    bwd_group(0)
    bwd_group(1)
    send_bwd(0, 0, 1)

    lap = GROUPS // CHUNKS

    @pl.loop(2, lap + 1)
    def _(g):
        bwd_group(g)
        send_bwd(g - 1, 0)

    for c in range(1, EARLY):

        @pl.loop(c * lap + 1, (c + 1) * lap + 1)
        def _(g):
            bwd_group(g)
            send_bwd(g - 1, c)

    others = pl.ds(1, 63)
    idx_copy(others, 1).wait()
    pair_copy().start()

    for k in range(SLOTS):
        bwd_0[0, k] = sbwd[0, k]

    pair_copy().wait()
    weight = jnp.zeros((1, 128), jnp.int32)
    for k in range(SLOTS):
        weight = jnp.where(lane == core * SLOTS + k, 128**k, weight)

    def rad_group(g):
        for j in range(GRP):
            s = g * GRP + j
            oc, m = index_spot(s)
            packed = jnp.sum(idx_in[oc, m] * weight)
            for k in range(SLOTS):
                srad[s, k] = rad[lax.rem(lax.div(packed, 128**k), 64)]

    rad_group(0)
    rad_group(1)
    send_rad(0, 0, 1)

    @pl.loop(2, lap + 1)
    def _(g):
        rad_group(g)
        send_rad(g - 1, 0)

    for c in range(1, CHUNKS):

        @pl.loop(c * lap + 1, min((c + 1) * lap + 1, GROUPS))
        def _(g):
            rad_group(g)
            send_rad(g - 1, c)

    for k in range(SLOTS):
        rrad[0, k] = srad[0, k]
    send_rad(GROUPS - 1, CHUNKS - 1)


    @pl.loop(EARLY * lap + 1, GROUPS)
    def _(g):
        bwd_group(g)


    def order(ids, which, c, base):
        block = ids[pl.ds(c * PER, PER)].reshape(PER, 128)
        parts = []
        for k in range(SLOTS):
            low = block[:, k : k + 1]
            high = block[:, SLOTS + k : SLOTS + k + 1]
            parts.append(jnp.broadcast_to(low + which * (high - low), (PER, 128)))
        q = jnp.concatenate(parts, axis=0)
        lanes = lax.broadcasted_iota(jnp.int32, (128, 128), 1)
        key = q * 128 + lax.broadcasted_iota(jnp.int32, (128, 128), 0)
        rank = jnp.sum((key.T < key).astype(jnp.int32), axis=1, keepdims=True)
        meta_v[base, 2 * c] = jnp.sum(jnp.where(rank == lanes, key, 0), axis=0, keepdims=True)
        upto = jnp.sum((q <= lanes).astype(jnp.int32), axis=0, keepdims=True)
        below = jnp.sum((q < lanes).astype(jnp.int32), axis=0, keepdims=True)
        meta_v[base, 2 * c + 1] = jnp.where(upto > below, upto, 0)

    def meta_copy(i):
        return pltpu.make_async_copy(meta_v.at[i], meta_s.at[i], msem.at[i])

    fill(tidx, tgt_s)

    @pl.loop(0, CHUNKS)
    def _(c):
        order(tidx, 0, c, 0)

    meta_copy(0).start()

    @pl.loop(0, GROUPS)
    def _(g):
        for j in range(GRP):
            s = g * GRP + j
            oc, m = index_spot(s)
            ridx[s] = idx_in[oc, m]

    @pl.loop(0, CHUNKS)
    def _(c):
        order(ridx, core, c, 1)

    meta_copy(1).start()

    seq[0] = jnp.zeros((16, 128), jnp.float32)
    gat[...] = jnp.zeros_like(gat)
    ret[...] = jnp.zeros_like(ret)

    def scan(values, offset, finish, c, base):
        def body(i, carry):
            acc, last = carry
            for j in range(8):
                n = i * 8 + j
                key = meta_s[base, 2 * c, 0, n]
                q = lax.div(key, 128)
                item = lax.rem(key, 128)
                x = values[offset + lax.rem(item, PER), lax.div(item, PER)].astype(jnp.float32)
                acc = acc * jnp.where(q == last, 1.0, 0.0) + x
                seq[n + 1] = acc
                last = q
            return acc, last

        lax.fori_loop(0, 16, body, (jnp.zeros((16, 128), jnp.float32), jnp.int32(-1)))

        @pl.loop(0, 16)
        def _(i):
            for j in range(4):
                t = i * 4 + j
                finish(t, seq[meta_s[base, 2 * c + 1, 0, t]])

    def to_gat(t, part):
        gat[t] += part

    def to_ret(t, part):
        ret[t] += part

    def to_irr(t, part):
        irr[t] = gat[t] + (ret[t] + part) / area[pl.ds(t, 1), :]

    meta_copy(0).wait()

    for c in range(CHUNKS):
        rad_rest(c).wait_recv()

        @pl.loop(c * lap, (c + 1) * lap)
        def _(g):
            fwd_group(g)

        scan(fwd, c * PER, to_gat, c, 0)

        if EARLY + c < CHUNKS:

            @pl.loop((EARLY + c) * lap, (EARLY + c + 1) * lap)
            def _(g):
                send_bwd(g, EARLY + c)

    meta_copy(1).wait()

    for c in range(CHUNKS):
        bwd_rest(c).wait_recv()
        scan(bwd_in[c], 0, to_ret if c < CHUNKS - 1 else to_irr, c, 1)

    bwd_rest(0).wait_send()
    bwd_rest(1).wait_send()
    bwd_rest(2).wait_send()
    bwd_rest(3).wait_send()
    rad_rest(0).wait_send()
    rad_rest(1).wait_send()
    rad_rest(2).wait_send()
    rad_rest(3).wait_send()


def shards(
    radiance, emission, reflectance, patch_area, form_factor,
    source_index, target_index, block_index, valid_count,
):
    hbm = pl.BlockSpec(memory_space=pltpu.HBM)
    vmem = pl.BlockSpec(memory_space=pltpu.VMEM)
    slab = (DEV, SLOTS, 16, 128)
    rows = (DEV, 1, 128)
    dma = pltpu.SemaphoreType.DMA
    irr = pl.pallas_call(
        exchange_kernel,
        out_shape=jax.ShapeDtypeStruct((64, 16, 128), jnp.float32),
        in_specs=[hbm] * 7,
        out_specs=vmem,
        scratch_shapes=[
            pltpu.SMEM((1, 512), jnp.int32),
            pltpu.SMEM((1, 512), jnp.int32),
            pltpu.SMEM((1, 512), jnp.int32),
            pltpu.SMEM((1, 128), jnp.int32),
            pltpu.VMEM((64, 16, 128), jnp.bfloat16),
            pltpu.VMEM((64, 128), jnp.float32),
            pltpu.VMEM((512, 128, 128), jnp.bfloat16),
            pltpu.VMEM((64, 16, 128), jnp.bfloat16),
            pltpu.VMEM(slab, jnp.bfloat16),
            *[pltpu.VMEM((PER, SLOTS, 16, 128), jnp.bfloat16) for _ in range(CHUNKS)],
            pltpu.VMEM(slab, jnp.bfloat16),
            pltpu.VMEM(slab, jnp.bfloat16),
            pltpu.VMEM(slab, jnp.float32),
            pltpu.VMEM((64, 1, 128), jnp.int32),
            pltpu.VMEM((2, 64, 1, 128), jnp.int32),
            pltpu.VMEM(rows, jnp.int32),
            pltpu.VMEM(rows, jnp.int32),
            pltpu.VMEM((136, 16, 128), jnp.float32),
            pltpu.VMEM((64, 16, 128), jnp.float32),
            pltpu.VMEM((64, 16, 128), jnp.float32),
            pltpu.VMEM((2, 2 * CHUNKS, 1, 128), jnp.int32),
            pltpu.SMEM((2, 2 * CHUNKS, 1, 128), jnp.int32),
            dma((6,)), dma((FCH,)), dma((2,)), dma, dma, dma, dma, dma((CHUNKS,)), dma((CHUNKS,)), dma((CHUNKS,)), dma((CHUNKS,)),
        ],
        compiler_params=pltpu.CompilerParams(
            collective_id=0, has_side_effects=True, vmem_limit_bytes=48 << 20
        ),
        name="exchange",
    )(
        *[pltpu.with_memory_space_constraint(v, pltpu.HBM) for v in (source_index, target_index, block_index, valid_count, radiance, patch_area, form_factor)]
    )
    return emission + reflectance * irr


def solution(mesh):
    both = ("gx", "gy")
    in_specs = (
        P(both, None, None),
        P(both, None, None),
        P(both, None, None),
        P(both, None),
        P(both, None, None),
        P(both, None),
        P(both, None),
        P(both, None),
        P(both, None),
    )
    return jax.shard_map(
        shards, mesh=mesh, in_specs=in_specs, out_specs=P(both, None, None), check_vma=False
    )
```

```python
import jax
import jax.numpy as jnp
from jax import lax
from jax.experimental import pallas as pl
from jax.experimental.pallas import tpu as pltpu
from jax.sharding import PartitionSpec as P

MESH = pl.DeviceIdType.MESH
DEV = 128
SLOTS = 4
GROUPS = 32
GRP = DEV // GROUPS
EARLY = 2
CHUNKS = 4
PER = DEV // CHUNKS
FCH = 8
MIX = 13


def position():
    z = lax.axis_index("gx")
    g = lax.axis_index("gy")
    y = lax.div(g, 8)
    x = lax.rem(lax.div(g, 2), 4)
    c = lax.rem(g, 2)
    return z, y, x, c


def peer(me, step, sign):
    z, y, x, c = me
    mixed = lax.rem(step * MIX, DEV)
    oc = lax.rem(mixed, 2)
    ox = lax.rem(lax.div(mixed, 2), 4)
    oy = lax.rem(lax.div(mixed, 8), 4)
    oz = lax.div(mixed, 32)
    z2 = lax.rem(z + 4 + sign * oz, 4)
    y2 = lax.rem(y + 4 + sign * oy, 4)
    x2 = lax.rem(x + 4 + sign * ox, 4)
    c2 = lax.rem(c + oc, 2)
    return z2, y2 * 8 + x2 * 2 + c2


def index_spot(step):
    mixed = lax.rem(step * MIX, DEV)
    return lax.rem(mixed, 2), lax.div(mixed, 2)


def chip(me, m):
    z, y, x, _ = me
    return (
        lax.rem(z + lax.div(m, 16), 4),
        lax.rem(y + lax.rem(lax.div(m, 4), 4), 4) * 8 + lax.rem(x + lax.rem(m, 4), 4) * 2,
    )


def exchange_kernel(
    src_h, tgt_h, blk_h, val_h, rad_h, area_h, f_h,
    irr,
    src_s, tgt_s, blk_s, val_s, rad, area,
    fv, wtd, sbwd, bwd_0, bwd_1, bwd_2, bwd_3, srad, rrad, fwd, sidx, idx_in, tidx, ridx, seq, gat, ret,
    meta_v, meta_s,
    lsem, fsem, msem, idx_send, idx_recv, pair_send, pair_recv, bwd_send, bwd_recv, rad_send, rad_recv,
):
    me = position()
    bwd_in = (bwd_0, bwd_1, bwd_2, bwd_3)

    loads = [
        pltpu.make_async_copy(a, b, lsem.at[i])
        for i, (a, b) in enumerate(
            [(src_h, src_s), (tgt_h, tgt_s), (blk_h, blk_s), (val_h, val_s), (rad_h, rad), (area_h, area)]
        )
    ]
    for load in loads:
        load.start()

    def f_copy(i):
        rows = pl.ds(i * (512 // FCH), 512 // FCH)
        return pltpu.make_async_copy(f_h.at[rows], fv.at[rows], fsem.at[i])

    for i in range(FCH):
        f_copy(i).start()

    barrier = pltpu.get_barrier_semaphore()

    def by_peer(step):
        for s in range(1, GRP):
            step(s)

        @pl.loop(1, GROUPS)
        def _(g):
            for j in range(GRP):
                step(g * GRP + j)

    by_peer(
        lambda s: pl.semaphore_signal(barrier, inc=1, device_id=peer(me, s, 1), device_id_type=MESH)
    )

    for load in loads:
        load.wait()

    lane = lax.broadcasted_iota(jnp.int32, (1, 128), 1)

    def fill(rows, table):
        @pl.loop(0, GROUPS)
        def _(g):
            for j in range(GRP):
                s = g * GRP + j
                z2, g2 = peer(me, s, 1)
                p = z2 * 32 + g2
                live = val_s[0, p]
                row = jnp.zeros((1, 128), jnp.int32)
                for k in range(SLOTS):
                    row = jnp.where(lane == k, table[0, p * SLOTS + k] + jnp.where(k < live, 0, 64), row)
                rows[s] = row

    @pl.loop(0, 32)
    def _(i):
        for j in range(2):
            m = i * 2 + j
            z2, g2 = chip(me, m)
            row = jnp.zeros((1, 128), jnp.int32)
            for c in range(2):
                p = z2 * 32 + g2 + c
                live = val_s[0, p]
                for k in range(SLOTS):
                    q = src_s[0, p * SLOTS + k] + jnp.where(k < live, 0, 64)
                    row = jnp.where(lane == c * SLOTS + k, q, row)
            sidx[m] = row

    idx_in[0, 0] = sidx[0]

    @pl.loop(0, 16)
    def _(i):
        for j in range(4):
            c = i * 4 + j
            wtd[c] = (area[pl.ds(c, 1), :] * rad[c].astype(jnp.float32)).astype(jnp.bfloat16)

    pl.semaphore_wait(barrier, DEV - 1)

    core = me[3]

    def idx_copy(rows, m):
        z2, g2 = chip(me, m)
        return pltpu.make_async_remote_copy(
            src_ref=sidx.at[rows], dst_ref=idx_in.at[0, rows], send_sem=idx_send, recv_sem=idx_recv,
            device_id=(z2, g2 + core), device_id_type=MESH,
        )

    def pair_copy():
        z2, g2 = chip(me, 0)
        return pltpu.make_async_remote_copy(
            src_ref=idx_in.at[0], dst_ref=idx_in.at[1], send_sem=pair_send, recv_sem=pair_recv,
            device_id=(z2, g2 + 1 - core), device_id_type=MESH,
        )

    for m in range(1, 3):
        idx_copy(m, m).start()

    @pl.loop(1, 21)
    def _(i):
        for j in range(3):
            m = i * 3 + j
            idx_copy(m, m).start()

    idx_copy(63, 63).start()

    def bwd_copy(first, count, s, c):
        return pltpu.make_async_remote_copy(
            src_ref=sbwd.at[pl.ds(first, count)],
            dst_ref=bwd_in[c].at[pl.ds(first - c * PER, count)],
            send_sem=bwd_send.at[c], recv_sem=bwd_recv.at[c],
            device_id=peer(me, s, 1), device_id_type=MESH,
        )

    def bwd_rest(c):
        first = max(1, c * PER)
        return bwd_copy(first, (c + 1) * PER - first, 1, c)

    def rad_copy(rows, s, c):
        return pltpu.make_async_remote_copy(
            src_ref=srad.at[rows], dst_ref=rrad.at[rows], send_sem=rad_send.at[c],
            recv_sem=rad_recv.at[c], device_id=peer(me, s, -1), device_id_type=MESH,
        )

    def rad_rest(c):
        first = max(1, c * PER)
        return rad_copy(pl.ds(first, (c + 1) * PER - first), 1, c)

    def send_rad(g, c, first=0):
        for j in range(first, GRP):
            s = g * GRP + j
            rad_copy(s, s, c).start()

    def send_bwd(g, c, first=0):
        for j in range(first, GRP):
            s = g * GRP + j
            bwd_copy(s, 1, s, c).start()

    def bwd_group(g):
        for j in range(GRP):
            s = g * GRP + j
            z2, g2 = peer(me, s, 1)
            base = (z2 * 32 + g2) * SLOTS
            for k in range(0, SLOTS, 2):
                w = jnp.concatenate([wtd[tgt_s[0, base + k]], wtd[tgt_s[0, base + k + 1]]], axis=0)
                f = jnp.concatenate([fv[blk_s[0, base + k]], fv[blk_s[0, base + k + 1]]], axis=1)
                r = jnp.dot(w, f, preferred_element_type=jnp.float32)
                sbwd[s, k] = r[:16, :128].astype(jnp.bfloat16)
                sbwd[s, k + 1] = r[16:, 128:].astype(jnp.bfloat16)

    def fwd_group(g):
        for j in range(GRP):
            s = g * GRP + j
            z2, g2 = peer(me, s, 1)
            base = (z2 * 32 + g2) * SLOTS
            for k in range(0, SLOTS, 2):
                v = jnp.concatenate([rrad[s, k], rrad[s, k + 1]], axis=0)
                f = jnp.concatenate([fv[blk_s[0, base + k]], fv[blk_s[0, base + k + 1]]], axis=0)
                r = lax.dot_general(v, f, (((1,), (1,)), ((), ())), preferred_element_type=jnp.float32)
                fwd[s, k] = r[:16, :128]
                fwd[s, k + 1] = r[16:, 128:]

    for i in range(FCH):
        f_copy(i).wait()

    bwd_group(0)
    bwd_group(1)
    send_bwd(0, 0, 1)

    lap = GROUPS // CHUNKS

    @pl.loop(2, lap + 1)
    def _(g):
        bwd_group(g)
        send_bwd(g - 1, 0)

    for c in range(1, EARLY):

        @pl.loop(c * lap + 1, (c + 1) * lap + 1)
        def _(g):
            bwd_group(g)
            send_bwd(g - 1, c)

    others = pl.ds(1, 63)
    idx_copy(others, 1).wait()
    pair_copy().start()

    for k in range(SLOTS):
        bwd_0[0, k] = sbwd[0, k]

    pair_copy().wait()
    weight = jnp.zeros((1, 128), jnp.int32)
    for k in range(SLOTS):
        weight = jnp.where(lane == core * SLOTS + k, 128**k, weight)

    def rad_group(g):
        for j in range(GRP):
            s = g * GRP + j
            oc, m = index_spot(s)
            packed = jnp.sum(idx_in[oc, m] * weight)
            for k in range(SLOTS):
                srad[s, k] = rad[jnp.bitwise_and(jnp.right_shift(packed, 7 * k), 63)]

    rad_group(0)
    rad_group(1)
    send_rad(0, 0, 1)

    @pl.loop(2, lap + 1)
    def _(g):
        rad_group(g)
        send_rad(g - 1, 0)

    for c in range(1, CHUNKS):

        @pl.loop(c * lap + 1, min((c + 1) * lap + 1, GROUPS))
        def _(g):
            rad_group(g)
            send_rad(g - 1, c)

    for k in range(SLOTS):
        rrad[0, k] = srad[0, k]
    send_rad(GROUPS - 1, CHUNKS - 1)


    @pl.loop(EARLY * lap + 1, GROUPS)
    def _(g):
        bwd_group(g)


    for c in range(EARLY, CHUNKS):

        @pl.loop(c * lap, (c + 1) * lap)
        def _(g):
            send_bwd(g, c)

    def order(ids, which, c, base):
        block = ids[pl.ds(c * PER, PER)].reshape(PER, 128)
        parts = []
        for k in range(SLOTS):
            low = block[:, k : k + 1]
            high = block[:, SLOTS + k : SLOTS + k + 1]
            parts.append(jnp.broadcast_to(low + which * (high - low), (PER, 128)))
        q = jnp.concatenate(parts, axis=0)
        lanes = lax.broadcasted_iota(jnp.int32, (128, 128), 1)
        key = q * 128 + lax.broadcasted_iota(jnp.int32, (128, 128), 0)
        rank = jnp.sum((key.T < key).astype(jnp.int32), axis=1, keepdims=True)
        meta_v[base, 2 * c] = jnp.sum(jnp.where(rank == lanes, key, 0), axis=0, keepdims=True)
        upto = jnp.sum((q <= lanes).astype(jnp.int32), axis=0, keepdims=True)
        below = jnp.sum((q < lanes).astype(jnp.int32), axis=0, keepdims=True)
        meta_v[base, 2 * c + 1] = jnp.where(upto > below, upto, 0)

    def meta_copy(i):
        return pltpu.make_async_copy(meta_v.at[i], meta_s.at[i], msem.at[i])

    fill(tidx, tgt_s)

    @pl.loop(0, CHUNKS)
    def _(c):
        order(tidx, 0, c, 0)

    meta_copy(0).start()

    @pl.loop(0, GROUPS)
    def _(g):
        for j in range(GRP):
            s = g * GRP + j
            oc, m = index_spot(s)
            ridx[s] = idx_in[oc, m]

    @pl.loop(0, CHUNKS)
    def _(c):
        order(ridx, core, c, 1)

    meta_copy(1).start()

    seq[0] = jnp.zeros((16, 128), jnp.float32)
    gat[...] = jnp.zeros_like(gat)
    ret[...] = jnp.zeros_like(ret)

    def scan(values, offset, finish, c, base):
        def body(i, carry):
            acc, last = carry
            for j in range(8):
                n = i * 8 + j
                key = meta_s[base, 2 * c, 0, n]
                q = jnp.right_shift(key, 7)
                item = jnp.bitwise_and(key, 127)
                row = jnp.bitwise_and(item, PER - 1)
                slot = jnp.right_shift(item, 5)
                x = values[offset + row, slot].astype(jnp.float32)
                acc = acc * jnp.where(q == last, 1.0, 0.0) + x
                seq[n + 1] = acc
                last = q
            return acc, last

        lax.fori_loop(0, 16, body, (jnp.zeros((16, 128), jnp.float32), jnp.int32(-1)))

        @pl.loop(0, 16)
        def _(i):
            for j in range(4):
                t = i * 4 + j
                finish(t, seq[meta_s[base, 2 * c + 1, 0, t]])

    def to_gat(t, part):
        gat[t] += part

    def to_ret(t, part):
        ret[t] += part

    def to_irr(t, part):
        irr[t] = gat[t] + (ret[t] + part) / area[pl.ds(t, 1), :]

    meta_copy(0).wait()

    for c in range(CHUNKS):
        rad_rest(c).wait_recv()

        @pl.loop(c * lap, (c + 1) * lap)
        def _(g):
            fwd_group(g)

        scan(fwd, c * PER, to_gat, c, 0)

    meta_copy(1).wait()

    for c in range(CHUNKS):
        bwd_rest(c).wait_recv()
        scan(bwd_in[c], 0, to_ret if c < CHUNKS - 1 else to_irr, c, 1)

    bwd_rest(0).wait_send()
    bwd_rest(1).wait_send()
    bwd_rest(2).wait_send()
    bwd_rest(3).wait_send()
    rad_rest(0).wait_send()
    rad_rest(1).wait_send()
    rad_rest(2).wait_send()
    rad_rest(3).wait_send()


def shards(
    radiance, emission, reflectance, patch_area, form_factor,
    source_index, target_index, block_index, valid_count,
):
    hbm = pl.BlockSpec(memory_space=pltpu.HBM)
    vmem = pl.BlockSpec(memory_space=pltpu.VMEM)
    slab = (DEV, SLOTS, 16, 128)
    rows = (DEV, 1, 128)
    dma = pltpu.SemaphoreType.DMA
    irr = pl.pallas_call(
        exchange_kernel,
        out_shape=jax.ShapeDtypeStruct((64, 16, 128), jnp.float32),
        in_specs=[hbm] * 7,
        out_specs=vmem,
        scratch_shapes=[
            pltpu.SMEM((1, 512), jnp.int32),
            pltpu.SMEM((1, 512), jnp.int32),
            pltpu.SMEM((1, 512), jnp.int32),
            pltpu.SMEM((1, 128), jnp.int32),
            pltpu.VMEM((64, 16, 128), jnp.bfloat16),
            pltpu.VMEM((64, 128), jnp.float32),
            pltpu.VMEM((512, 128, 128), jnp.bfloat16),
            pltpu.VMEM((64, 16, 128), jnp.bfloat16),
            pltpu.VMEM(slab, jnp.bfloat16),
            *[pltpu.VMEM((PER, SLOTS, 16, 128), jnp.bfloat16) for _ in range(CHUNKS)],
            pltpu.VMEM(slab, jnp.bfloat16),
            pltpu.VMEM(slab, jnp.bfloat16),
            pltpu.VMEM(slab, jnp.float32),
            pltpu.VMEM((64, 1, 128), jnp.int32),
            pltpu.VMEM((2, 64, 1, 128), jnp.int32),
            pltpu.VMEM(rows, jnp.int32),
            pltpu.VMEM(rows, jnp.int32),
            pltpu.VMEM((136, 16, 128), jnp.float32),
            pltpu.VMEM((64, 16, 128), jnp.float32),
            pltpu.VMEM((64, 16, 128), jnp.float32),
            pltpu.VMEM((2, 2 * CHUNKS, 1, 128), jnp.int32),
            pltpu.SMEM((2, 2 * CHUNKS, 1, 128), jnp.int32),
            dma((6,)), dma((FCH,)), dma((2,)), dma, dma, dma, dma, dma((CHUNKS,)), dma((CHUNKS,)), dma((CHUNKS,)), dma((CHUNKS,)),
        ],
        compiler_params=pltpu.CompilerParams(
            collective_id=0, has_side_effects=True, vmem_limit_bytes=48 << 20
        ),
        name="exchange",
    )(
        *[pltpu.with_memory_space_constraint(v, pltpu.HBM) for v in (source_index, target_index, block_index, valid_count, radiance, patch_area, form_factor)]
    )
    return emission + reflectance * irr


def solution(mesh):
    both = ("gx", "gy")
    in_specs = (
        P(both, None, None),
        P(both, None, None),
        P(both, None, None),
        P(both, None),
        P(both, None, None),
        P(both, None),
        P(both, None),
        P(both, None),
        P(both, None),
    )
    return jax.shard_map(
        shards, mesh=mesh, in_specs=in_specs, out_specs=P(both, None, None), check_vma=False
    )
```

```python
import jax
import jax.numpy as jnp
from jax import lax
from jax.experimental import pallas as pl
from jax.experimental.pallas import tpu as pltpu
from jax.sharding import PartitionSpec as P

MESH = pl.DeviceIdType.MESH
DEV = 128
SLOTS = 4
GROUPS = 32
GRP = DEV // GROUPS
EARLY = 2
CHUNKS = 4
PER = DEV // CHUNKS
FCH = 2
MIX = 13


def position():
    z = lax.axis_index("gx")
    g = lax.axis_index("gy")
    y = lax.div(g, 8)
    x = lax.rem(lax.div(g, 2), 4)
    c = lax.rem(g, 2)
    return z, y, x, c


def peer(me, step, sign):
    z, y, x, c = me
    mixed = lax.rem(step * MIX, DEV)
    oc = lax.rem(mixed, 2)
    ox = lax.rem(lax.div(mixed, 2), 4)
    oy = lax.rem(lax.div(mixed, 8), 4)
    oz = lax.div(mixed, 32)
    z2 = lax.rem(z + 4 + sign * oz, 4)
    y2 = lax.rem(y + 4 + sign * oy, 4)
    x2 = lax.rem(x + 4 + sign * ox, 4)
    c2 = lax.rem(c + oc, 2)
    return z2, y2 * 8 + x2 * 2 + c2


def index_spot(step):
    mixed = lax.rem(step * MIX, DEV)
    return lax.rem(mixed, 2), lax.div(mixed, 2)


def chip(me, m):
    z, y, x, _ = me
    return (
        lax.rem(z + lax.div(m, 16), 4),
        lax.rem(y + lax.rem(lax.div(m, 4), 4), 4) * 8 + lax.rem(x + lax.rem(m, 4), 4) * 2,
    )


def exchange_kernel(
    src_h, tgt_h, blk_h, val_h, rad_h, area_h, f_h,
    irr,
    src_s, tgt_s, blk_s, val_s, rad, area,
    fv, wtd, sbwd, bwd_0, bwd_1, bwd_2, bwd_3, srad, rrad, fwd, sidx, idx_in, tidx, ridx, seq, gat, ret,
    meta_v, meta_s,
    lsem, fsem, msem, idx_send, idx_recv, pair_send, pair_recv, bwd_send, bwd_recv, rad_send, rad_recv,
):
    me = position()
    bwd_in = (bwd_0, bwd_1, bwd_2, bwd_3)

    loads = [
        pltpu.make_async_copy(a, b, lsem.at[i])
        for i, (a, b) in enumerate(
            [(src_h, src_s), (tgt_h, tgt_s), (blk_h, blk_s), (val_h, val_s), (rad_h, rad), (area_h, area)]
        )
    ]
    for load in loads:
        load.start()

    def f_copy(i):
        rows = pl.ds(i * (512 // FCH), 512 // FCH)
        return pltpu.make_async_copy(f_h.at[rows], fv.at[rows], fsem.at[i])

    for i in range(FCH):
        f_copy(i).start()

    barrier = pltpu.get_barrier_semaphore()

    def by_peer(step):
        for s in range(1, GRP):
            step(s)

        @pl.loop(1, GROUPS)
        def _(g):
            for j in range(GRP):
                step(g * GRP + j)

    by_peer(
        lambda s: pl.semaphore_signal(barrier, inc=1, device_id=peer(me, s, 1), device_id_type=MESH)
    )

    for load in loads:
        load.wait()

    lane = lax.broadcasted_iota(jnp.int32, (1, 128), 1)

    def fill(rows, table):
        @pl.loop(0, GROUPS)
        def _(g):
            for j in range(GRP):
                s = g * GRP + j
                z2, g2 = peer(me, s, 1)
                p = z2 * 32 + g2
                live = val_s[0, p]
                row = jnp.zeros((1, 128), jnp.int32)
                for k in range(SLOTS):
                    row = jnp.where(lane == k, table[0, p * SLOTS + k] + jnp.where(k < live, 0, 64), row)
                rows[s] = row

    @pl.loop(0, 32)
    def _(i):
        for j in range(2):
            m = i * 2 + j
            z2, g2 = chip(me, m)
            row = jnp.zeros((1, 128), jnp.int32)
            for c in range(2):
                p = z2 * 32 + g2 + c
                live = val_s[0, p]
                for k in range(SLOTS):
                    q = src_s[0, p * SLOTS + k] + jnp.where(k < live, 0, 64)
                    row = jnp.where(lane == c * SLOTS + k, q, row)
            sidx[m] = row

    idx_in[0, 0] = sidx[0]

    @pl.loop(0, 16)
    def _(i):
        for j in range(4):
            c = i * 4 + j
            wtd[c] = (area[pl.ds(c, 1), :] * rad[c].astype(jnp.float32)).astype(jnp.bfloat16)

    pl.semaphore_wait(barrier, DEV - 1)

    core = me[3]

    def idx_copy(rows, m):
        z2, g2 = chip(me, m)
        return pltpu.make_async_remote_copy(
            src_ref=sidx.at[rows], dst_ref=idx_in.at[0, rows], send_sem=idx_send, recv_sem=idx_recv,
            device_id=(z2, g2 + core), device_id_type=MESH,
        )

    def pair_copy():
        z2, g2 = chip(me, 0)
        return pltpu.make_async_remote_copy(
            src_ref=idx_in.at[0], dst_ref=idx_in.at[1], send_sem=pair_send, recv_sem=pair_recv,
            device_id=(z2, g2 + 1 - core), device_id_type=MESH,
        )

    for m in range(1, 3):
        idx_copy(m, m).start()

    @pl.loop(1, 21)
    def _(i):
        for j in range(3):
            m = i * 3 + j
            idx_copy(m, m).start()

    idx_copy(63, 63).start()

    def bwd_copy(first, count, s, c):
        return pltpu.make_async_remote_copy(
            src_ref=sbwd.at[pl.ds(first, count)],
            dst_ref=bwd_in[c].at[pl.ds(first - c * PER, count)],
            send_sem=bwd_send.at[c], recv_sem=bwd_recv.at[c],
            device_id=peer(me, s, 1), device_id_type=MESH,
        )

    def bwd_rest(c):
        first = max(1, c * PER)
        return bwd_copy(first, (c + 1) * PER - first, 1, c)

    def rad_copy(rows, s, c):
        return pltpu.make_async_remote_copy(
            src_ref=srad.at[rows], dst_ref=rrad.at[rows], send_sem=rad_send.at[c],
            recv_sem=rad_recv.at[c], device_id=peer(me, s, -1), device_id_type=MESH,
        )

    def rad_rest(c):
        first = max(1, c * PER)
        return rad_copy(pl.ds(first, (c + 1) * PER - first), 1, c)

    def send_rad(g, c, first=0):
        for j in range(first, GRP):
            s = g * GRP + j
            rad_copy(s, s, c).start()

    def send_bwd(g, c, first=0):
        for j in range(first, GRP):
            s = g * GRP + j
            bwd_copy(s, 1, s, c).start()

    def bwd_group(g):
        for j in range(GRP):
            s = g * GRP + j
            z2, g2 = peer(me, s, 1)
            base = (z2 * 32 + g2) * SLOTS
            for k in range(0, SLOTS, 2):
                w = jnp.concatenate([wtd[tgt_s[0, base + k]], wtd[tgt_s[0, base + k + 1]]], axis=0)
                f = jnp.concatenate([fv[blk_s[0, base + k]], fv[blk_s[0, base + k + 1]]], axis=1)
                r = jnp.dot(w, f, preferred_element_type=jnp.float32)
                sbwd[s, k] = r[:16, :128].astype(jnp.bfloat16)
                sbwd[s, k + 1] = r[16:, 128:].astype(jnp.bfloat16)

    def fwd_group(g):
        for j in range(GRP):
            s = g * GRP + j
            z2, g2 = peer(me, s, 1)
            base = (z2 * 32 + g2) * SLOTS
            for k in range(0, SLOTS, 2):
                v = jnp.concatenate([rrad[s, k], rrad[s, k + 1]], axis=0)
                f = jnp.concatenate([fv[blk_s[0, base + k]], fv[blk_s[0, base + k + 1]]], axis=0)
                r = lax.dot_general(v, f, (((1,), (1,)), ((), ())), preferred_element_type=jnp.float32)
                fwd[s, k] = r[:16, :128]
                fwd[s, k + 1] = r[16:, 128:]

    for i in range(FCH):
        f_copy(i).wait()

    bwd_group(0)
    bwd_group(1)
    send_bwd(0, 0, 1)

    lap = GROUPS // CHUNKS

    @pl.loop(2, lap + 1)
    def _(g):
        bwd_group(g)
        send_bwd(g - 1, 0)

    for c in range(1, EARLY):

        @pl.loop(c * lap + 1, (c + 1) * lap + 1)
        def _(g):
            bwd_group(g)
            send_bwd(g - 1, c)

    others = pl.ds(1, 63)
    idx_copy(others, 1).wait()
    pair_copy().start()

    for k in range(SLOTS):
        bwd_0[0, k] = sbwd[0, k]

    pair_copy().wait()
    weight = jnp.zeros((1, 128), jnp.int32)
    for k in range(SLOTS):
        weight = jnp.where(lane == core * SLOTS + k, 128**k, weight)

    def rad_group(g):
        for j in range(GRP):
            s = g * GRP + j
            oc, m = index_spot(s)
            packed = jnp.sum(idx_in[oc, m] * weight)
            for k in range(SLOTS):
                srad[s, k] = rad[jnp.bitwise_and(jnp.right_shift(packed, 7 * k), 63)]

    rad_group(0)
    rad_group(1)
    send_rad(0, 0, 1)

    @pl.loop(2, lap + 1)
    def _(g):
        rad_group(g)
        send_rad(g - 1, 0)

    for c in range(1, CHUNKS):

        @pl.loop(c * lap + 1, min((c + 1) * lap + 1, GROUPS))
        def _(g):
            rad_group(g)
            send_rad(g - 1, c)

    for k in range(SLOTS):
        rrad[0, k] = srad[0, k]
    send_rad(GROUPS - 1, CHUNKS - 1)


    @pl.loop(EARLY * lap + 1, GROUPS)
    def _(g):
        bwd_group(g)


    for c in range(EARLY, CHUNKS):

        @pl.loop(c * lap, (c + 1) * lap)
        def _(g):
            send_bwd(g, c)

    def order(ids, which, c, base):
        block = ids[pl.ds(c * PER, PER)].reshape(PER, 128)
        parts = []
        for k in range(SLOTS):
            low = block[:, k : k + 1]
            high = block[:, SLOTS + k : SLOTS + k + 1]
            parts.append(jnp.broadcast_to(low + which * (high - low), (PER, 128)))
        q = jnp.concatenate(parts, axis=0)
        lanes = lax.broadcasted_iota(jnp.int32, (128, 128), 1)
        key = q * 128 + lax.broadcasted_iota(jnp.int32, (128, 128), 0)
        rank = jnp.sum((key.T < key).astype(jnp.int32), axis=1, keepdims=True)
        meta_v[base, 2 * c] = jnp.sum(jnp.where(rank == lanes, key, 0), axis=0, keepdims=True)
        upto = jnp.sum((q <= lanes).astype(jnp.int32), axis=0, keepdims=True)
        below = jnp.sum((q < lanes).astype(jnp.int32), axis=0, keepdims=True)
        meta_v[base, 2 * c + 1] = jnp.where(upto > below, upto, 0)

    def meta_copy(i):
        return pltpu.make_async_copy(meta_v.at[i], meta_s.at[i], msem.at[i])

    fill(tidx, tgt_s)

    @pl.loop(0, CHUNKS)
    def _(c):
        order(tidx, 0, c, 0)

    meta_copy(0).start()

    @pl.loop(0, GROUPS)
    def _(g):
        for j in range(GRP):
            s = g * GRP + j
            oc, m = index_spot(s)
            ridx[s] = idx_in[oc, m]

    @pl.loop(0, CHUNKS)
    def _(c):
        order(ridx, core, c, 1)

    meta_copy(1).start()

    seq[0] = jnp.zeros((16, 128), jnp.float32)
    gat[...] = jnp.zeros_like(gat)
    ret[...] = jnp.zeros_like(ret)

    def scan(values, offset, finish, c, base):
        def body(i, carry):
            acc, last = carry
            for j in range(8):
                n = i * 8 + j
                key = meta_s[base, 2 * c, 0, n]
                q = jnp.right_shift(key, 7)
                item = jnp.bitwise_and(key, 127)
                row = jnp.bitwise_and(item, PER - 1)
                slot = jnp.right_shift(item, 5)
                x = values[offset + row, slot].astype(jnp.float32)
                acc = acc * jnp.where(q == last, 1.0, 0.0) + x
                seq[n + 1] = acc
                last = q
            return acc, last

        lax.fori_loop(0, 16, body, (jnp.zeros((16, 128), jnp.float32), jnp.int32(-1)))

        @pl.loop(0, 16)
        def _(i):
            for j in range(4):
                t = i * 4 + j
                finish(t, seq[meta_s[base, 2 * c + 1, 0, t]])

    def to_gat(t, part):
        gat[t] += part

    def to_ret(t, part):
        ret[t] += part

    def to_irr(t, part):
        irr[t] = gat[t] + (ret[t] + part) / area[pl.ds(t, 1), :]

    meta_copy(0).wait()

    for c in range(CHUNKS):
        rad_rest(c).wait_recv()

        @pl.loop(c * lap, (c + 1) * lap)
        def _(g):
            fwd_group(g)

        scan(fwd, c * PER, to_gat, c, 0)

    meta_copy(1).wait()

    for c in range(CHUNKS):
        bwd_rest(c).wait_recv()
        scan(bwd_in[c], 0, to_ret if c < CHUNKS - 1 else to_irr, c, 1)

    bwd_rest(0).wait_send()
    bwd_rest(1).wait_send()
    bwd_rest(2).wait_send()
    bwd_rest(3).wait_send()
    rad_rest(0).wait_send()
    rad_rest(1).wait_send()
    rad_rest(2).wait_send()
    rad_rest(3).wait_send()


def shards(
    radiance, emission, reflectance, patch_area, form_factor,
    source_index, target_index, block_index, valid_count,
):
    hbm = pl.BlockSpec(memory_space=pltpu.HBM)
    vmem = pl.BlockSpec(memory_space=pltpu.VMEM)
    slab = (DEV, SLOTS, 16, 128)
    rows = (DEV, 1, 128)
    dma = pltpu.SemaphoreType.DMA
    irr = pl.pallas_call(
        exchange_kernel,
        out_shape=jax.ShapeDtypeStruct((64, 16, 128), jnp.float32),
        in_specs=[hbm] * 7,
        out_specs=vmem,
        scratch_shapes=[
            pltpu.SMEM((1, 512), jnp.int32),
            pltpu.SMEM((1, 512), jnp.int32),
            pltpu.SMEM((1, 512), jnp.int32),
            pltpu.SMEM((1, 128), jnp.int32),
            pltpu.VMEM((64, 16, 128), jnp.bfloat16),
            pltpu.VMEM((64, 128), jnp.float32),
            pltpu.VMEM((512, 128, 128), jnp.bfloat16),
            pltpu.VMEM((64, 16, 128), jnp.bfloat16),
            pltpu.VMEM(slab, jnp.bfloat16),
            *[pltpu.VMEM((PER, SLOTS, 16, 128), jnp.bfloat16) for _ in range(CHUNKS)],
            pltpu.VMEM(slab, jnp.bfloat16),
            pltpu.VMEM(slab, jnp.bfloat16),
            pltpu.VMEM(slab, jnp.float32),
            pltpu.VMEM((64, 1, 128), jnp.int32),
            pltpu.VMEM((2, 64, 1, 128), jnp.int32),
            pltpu.VMEM(rows, jnp.int32),
            pltpu.VMEM(rows, jnp.int32),
            pltpu.VMEM((136, 16, 128), jnp.float32),
            pltpu.VMEM((64, 16, 128), jnp.float32),
            pltpu.VMEM((64, 16, 128), jnp.float32),
            pltpu.VMEM((2, 2 * CHUNKS, 1, 128), jnp.int32),
            pltpu.SMEM((2, 2 * CHUNKS, 1, 128), jnp.int32),
            dma((6,)), dma((FCH,)), dma((2,)), dma, dma, dma, dma, dma((CHUNKS,)), dma((CHUNKS,)), dma((CHUNKS,)), dma((CHUNKS,)),
        ],
        compiler_params=pltpu.CompilerParams(
            collective_id=0, has_side_effects=True, vmem_limit_bytes=48 << 20
        ),
        name="exchange",
    )(
        *[pltpu.with_memory_space_constraint(v, pltpu.HBM) for v in (source_index, target_index, block_index, valid_count, radiance, patch_area, form_factor)]
    )
    return emission + reflectance * irr


def solution(mesh):
    both = ("gx", "gy")
    in_specs = (
        P(both, None, None),
        P(both, None, None),
        P(both, None, None),
        P(both, None),
        P(both, None, None),
        P(both, None),
        P(both, None),
        P(both, None),
        P(both, None),
    )
    return jax.shard_map(
        shards, mesh=mesh, in_specs=in_specs, out_specs=P(both, None, None), check_vma=False
    )
```
